128 devices in a mesh: section: 2 (over x_hi), gx: 16 (over z, y), gy: 4 (over x_lo, core).
Axes of the slice: x: 4 (x_hi: 2, x_lo: 2; x = x_hi * 2 + x_lo), y: 4, z: 4, core: 2. Of those that a mesh axis runs over, the one named last changes fastest.
Arguments:
- inputs: bfloat16 [4, 32, 8192], P(None, None, 'gx'), may hold values from -6 to 6
- gains: bfloat16 [2, 8192], P('section', 'gx'), may hold values from 0.5 to 1.5
- query_weight: bfloat16 [2, 8192, 16384], P('section', 'gx', 'gy'), may hold values from -0.0625 to 0.0625
- key_value_weight: bfloat16 [2, 8192, 2048], P('section', 'gx', 'gy'), may hold values from -0.0625 to 0.0625
- output_weight: bfloat16 [2, 16384, 8192], P('section', 'gy', 'gx'), may hold values from -0.375 to 0.375
- rotated_key_cache: bfloat16 [2, 4, 32, 8, 1024, 128], P('section', None, 'gx', 'gy'), may hold values from -600 to 600
- stored_value_cache: bfloat16 [2, 4, 32, 8, 1024, 128], P('section', None, 'gx', 'gy'), may hold values from -6 to 6
- lengths: int32 [4, 32], P(None, 'gx'), may hold values from 2 to 1024
Outputs:
- states: bfloat16 [2, 4, 32, 8192], P('section', None, None, ('gx', 'gy'))
The draws below stay inside these ranges and needn't reach their ends.
Inputs may be any that keep to these rules, and one draw needn't show every extreme that they name: The new token sits at position lengths; slots 0 to lengths - 1 are live.
All inputs are finite; a program needn't handle non-finite values.
Results may differ from the reference program's by a relative error of at most 0.015.
The reference program's roundings to bfloat16 on the way count: a program that leaves them out, or rounds other values in their place, can miss the bound.
Values may be sent and summed in bfloat16 or wider, within the bound.
A program may use at most 64 MiB of HBM per device.

```python
import jax
import jax.numpy as jnp
from jax import lax

MODEL_WIDTH = 8192
QUERY_HEADS = 128
KEY_VALUE_HEADS = 8
HEAD_SIZE = 128
CACHE_SLOTS = 1024
MICRO_BATCHES = 4
LAYER_COUNT = 2
MICRO_SEQUENCES = 32


def draw_rotated_key_cache(key, part):
    complete_shape = (LAYER_COUNT, MICRO_BATCHES, MICRO_SEQUENCES, KEY_VALUE_HEADS, CACHE_SLOTS, HEAD_SIZE)
    base_draw = jnp.clip(jax.random.normal(key, complete_shape, jnp.float32), -6.0, 6.0)
    return base_draw.astype(jnp.bfloat16)


def plant(values, stream_key, low, top_value):
    longest = values.shape.index(max(values.shape))
    spots = []
    for shift in (0, 1):
        where = [jax.random.randint(jax.random.fold_in(stream_key, axis), (), 0, length) for axis, length in enumerate(values.shape)]
        where[longest] = (where[longest] + shift) % values.shape[longest]
        spots.append(tuple(where))
    return values.at[spots[0]].set(low).at[spots[1]].set(top_value)


def shard_levels(rng, shape, shards, least, top_value):
    def one(dim, parts):
        heights = jax.random.uniform(jax.random.fold_in(jax.random.fold_in(rng, 6), dim), (parts,), jnp.float32, least / len(shards), top_value / len(shards))
        return jnp.repeat(jnp.exp(heights), shape[dim] // parts).reshape((-1,) + (1,) * (len(shape) - dim - 1))

    gain = one(*shards[0])
    for cut in shards[1:]:
        gain = gain * one(*cut)
    return gain


def gaussian(rng, shape, deviation, bound, split=(), kind=jnp.bfloat16):
    level = shard_levels(rng, shape, split, -0.22, 0.18) if split else 1.0
    array = jax.random.normal(rng, shape, jnp.float32) * deviation * level
    return jnp.minimum(jnp.maximum(array, -bound), bound).astype(kind)


def setup_inputs(seed: int = 0) -> dict:
    streams_of = jax.random.split(jax.random.key(seed), 9)
    return {
        "inputs": gaussian(streams_of[0], (MICRO_BATCHES, MICRO_SEQUENCES, MODEL_WIDTH), 1.0, 6.0, ((2, 16),)),
        "gains": jnp.clip(1.0 + 0.1 * jax.random.normal(streams_of[1], (LAYER_COUNT, MODEL_WIDTH), jnp.float32), 0.5, 1.5).astype(jnp.bfloat16),
        "query_weight": gaussian(streams_of[2], (LAYER_COUNT, MODEL_WIDTH, QUERY_HEADS * HEAD_SIZE), MODEL_WIDTH ** -0.5, 0.0625, ((0, 2), (1, 16), (2, 4))),
        "key_value_weight": gaussian(streams_of[3], (LAYER_COUNT, MODEL_WIDTH, KEY_VALUE_HEADS * 2 * HEAD_SIZE), MODEL_WIDTH ** -0.5, 0.0625, ((0, 2), (1, 16), (2, 4))),
        "output_weight": gaussian(streams_of[4], (LAYER_COUNT, QUERY_HEADS * HEAD_SIZE, MODEL_WIDTH), (QUERY_HEADS * HEAD_SIZE // 64) ** -0.5, 0.375, ((0, 2), (1, 4), (2, 16))),
        "rotated_key_cache": draw_rotated_key_cache(jax.random.fold_in(streams_of[8], 71), 0),
        "stored_value_cache": gaussian(streams_of[6], (LAYER_COUNT, MICRO_BATCHES, MICRO_SEQUENCES, KEY_VALUE_HEADS, CACHE_SLOTS, HEAD_SIZE), 1.0, 6.0, ((0, 2), (2, 16), (3, 4))),
        "lengths": plant(jax.random.randint(streams_of[7], (MICRO_BATCHES, MICRO_SEQUENCES), 2, CACHE_SLOTS + 1), jax.random.fold_in(streams_of[7], 1), 2, CACHE_SLOTS).astype(jnp.int32),
    }


ROPE_THETA = 500000.0
NORM_EPS = 1e-05

def rotate(vectors, positions):
    half_dim = vectors.shape[-1] // 2
    frequency = ROPE_THETA ** (-2.0 * jnp.arange(half_dim, dtype=jnp.float32) / vectors.shape[-1])
    angles = positions.astype(jnp.float32)[:, None] * frequency[None, :]
    cos_part = jnp.cos(angles)[:, None, :]
    sine_part = jnp.sin(angles)[:, None, :]
    front_half = vectors[..., :half_dim]
    back_half = vectors[..., half_dim:]
    return jnp.concatenate([front_half * cos_part - back_half * sine_part, back_half * cos_part + front_half * sine_part], axis=-1)

def layer_attention(hidden_state, gain_row, w_query, w_pairs, w_out, cached_keys, cached_values, sequence_lengths):
    every_row = hidden_state.shape[0]
    group_width = QUERY_HEADS // KEY_VALUE_HEADS
    widened = hidden_state.astype(jnp.float32)
    squares = lax.optimization_barrier(jnp.sum(widened * widened, axis=1))
    scaled = (widened * gain_row.astype(jnp.float32)).astype(jnp.bfloat16)
    factor = lax.rsqrt(squares / MODEL_WIDTH + NORM_EPS)
    query_rows = factor[:, None] * jnp.dot(scaled, w_query, preferred_element_type=jnp.float32)
    key_value_pairs = factor[:, None] * jnp.dot(scaled, w_pairs, preferred_element_type=jnp.float32)
    query_rows = rotate(query_rows.reshape(every_row, QUERY_HEADS, HEAD_SIZE), sequence_lengths).astype(jnp.bfloat16)
    key_value_pairs = key_value_pairs.reshape(every_row, KEY_VALUE_HEADS, 2, HEAD_SIZE)
    fresh_key = rotate(key_value_pairs[:, :, 0], sequence_lengths).astype(jnp.bfloat16)
    fresh_value = key_value_pairs[:, :, 1].astype(jnp.bfloat16)
    grouped_queries = query_rows.reshape(every_row, KEY_VALUE_HEADS, group_width, HEAD_SIZE).astype(jnp.float32)
    inv_scale = 1.0 / HEAD_SIZE ** 0.5
    scores = jnp.einsum('bhgd,bhtd->bhgt', grouped_queries, cached_keys.astype(jnp.float32)) * inv_scale
    self_score = jnp.einsum('bhgd,bhd->bhg', grouped_queries, fresh_key.astype(jnp.float32)) * inv_scale
    live_mask = jnp.arange(CACHE_SLOTS, dtype=jnp.int32)[None, None, None, :] < sequence_lengths[:, None, None, None]
    scores = jnp.where(live_mask, scores, -jnp.inf)
    row_top = jnp.maximum(lax.optimization_barrier(jnp.max(scores, axis=-1)), self_score)
    weights = jnp.exp(scores - row_top[..., None])
    own_weight = jnp.exp(self_score - row_top)
    denom_sum = lax.optimization_barrier(jnp.sum(weights, axis=-1)) + own_weight
    weights = (weights / denom_sum[..., None]).astype(jnp.bfloat16)
    own_weight = (own_weight / denom_sum).astype(jnp.bfloat16)
    mixed_vals = jnp.einsum('bhgt,bhtd->bhgd', weights.astype(jnp.float32), cached_values.astype(jnp.float32))
    mixed_vals = mixed_vals + own_weight.astype(jnp.float32)[..., None] * fresh_value.astype(jnp.float32)[:, :, None, :]
    head_out = mixed_vals.reshape(every_row, QUERY_HEADS * HEAD_SIZE).astype(jnp.bfloat16)
    branch = jnp.dot(head_out, w_out, preferred_element_type=jnp.float32)
    return (widened + branch).astype(jnp.bfloat16)

def reference(inputs, gains, query_weight, key_value_weight, output_weight, rotated_key_cache, stored_value_cache, lengths):
    every_row = MICRO_BATCHES * MICRO_SEQUENCES
    hidden_state = inputs.reshape(every_row, MODEL_WIDTH)
    sequence_lengths = lengths.reshape(every_row)
    layer_outs = []
    for layer_index in range(LAYER_COUNT):
        hidden_state = layer_attention(hidden_state, gains[layer_index], query_weight[layer_index], key_value_weight[layer_index], output_weight[layer_index], rotated_key_cache[layer_index].reshape(every_row, KEY_VALUE_HEADS, CACHE_SLOTS, HEAD_SIZE), stored_value_cache[layer_index].reshape(every_row, KEY_VALUE_HEADS, CACHE_SLOTS, HEAD_SIZE), sequence_lengths)
        layer_outs.append(hidden_state.reshape(MICRO_BATCHES, MICRO_SEQUENCES, MODEL_WIDTH))
    return jnp.stack(layer_outs)
```

```python
import functools

import jax
import jax.numpy as jnp
from jax import lax
from jax.experimental import pallas as pl
from jax.experimental.pallas import tpu as pltpu
from jax.sharding import PartitionSpec as P

MODEL_WIDTH = 8192
ROPE_THETA = 500000.0
NORM_EPS = 1e-05

MESH = pl.DeviceIdType.MESH
MICRO = 4
ROWS = 32
TILES = 19
LOW = 80
HIGH = 72
STAGES = 7


def swapped_rows(src, dst):
    for a in range(4):
        for b in range(4):
            dst[8 * b + 2 * a : 8 * b + 2 * a + 2, :] = src[8 * a + 2 * b : 8 * a + 2 * b + 2, :]


def kernel(
    x_hbm,
    gain_ref,
    rope_ref,
    len_ref,
    wq_hbm,
    wkv_hbm,
    wo_hbm,
    k_hbm,
    v_hbm,
    out_ref,
    xs,
    wq,
    wkv,
    wo,
    keys,
    values,
    wide,
    turned,
    part,
    lo2,
    lod,
    los,
    hi2,
    hid,
    his,
    whole,
    piece,
    piece_in,
    total,
    heads,
    spread,
    lhs_in,
    lhs,
    branch0,
    branch1,
    branch2,
    share,
    share_in,
    result,
    local_sem,
    s1_send,
    s1_recv,
    s2_send,
    s2_recv,
    g1_send,
    g1_recv,
    g2_send,
    g2_recv,
    gy_send,
    gy_recv,
    x_send,
    x_recv,
):
    sec = lax.axis_index("section")
    gx = lax.axis_index("gx")
    gy = lax.axis_index("gy")
    z = gx // 4
    y = gx % 4

    def along_z(k):
        return (sec, ((z + k) % 4) * 4 + y, gy)

    def along_y(k):
        return (sec, z * 4 + (y + k) % 4, gy)

    def along_gy(k):
        return (sec, gx, (gy + k) % 4)

    firsts = ((z, along_z), (y, along_y))
    seconds = ((y, along_y), (z, along_z))

    def remote(src, dst, send, recv, dev):
        return pltpu.make_async_remote_copy(
            src_ref=src, dst_ref=dst, send_sem=send, recv_sem=recv, device_id=dev, device_id_type=MESH
        )

    local = []

    def stage_in(src, dst):
        copy = pltpu.make_async_copy(src, dst, local_sem.at[len(local)])
        local.append(copy)
        return copy

    x_copies = [stage_in(x_hbm.at[:, :, pl.ds(128 * c, 128)], xs.at[:, c]) for c in range(4)]
    wq_copies = []
    wkv_copies = []
    for h in range(2):
        wq_copies.append(stage_in(wq_hbm.at[0, :, pl.ds(2048 * h, 2048)], wq.at[h]))
        wkv_copies.append(stage_in(wkv_hbm.at[0, :, pl.ds(256 * h, 256)], wkv.at[h]))
    k_copy = stage_in(k_hbm.at[0], keys)
    v_copy = stage_in(v_hbm.at[0], values)
    wo_copy = stage_in(wo_hbm.at[0], wo)

    @pl.when(sec == 0)
    def _():
        for copy in x_copies:
            copy.start()

    for h in range(2):
        wq_copies[h].start()
        wkv_copies[h].start()
    k_copy.start()
    v_copy.start()
    wo_copy.start()

    barrier = pltpu.get_barrier_semaphore()
    partners = [along_z(k) for k in (1, 2, 3)] + [along_y(k) for k in (1, 2, 3)]
    partners += [along_gy(k) for k in (1, 2, 3)]
    partners += [(1 - sec, gx, (gy + k) % 4) for k in range(4)]
    for dev in partners:
        pl.semaphore_signal(barrier, inc=1, device_id=dev, device_id_type=MESH)

    def first_copies(m, h):
        p, dev = firsts[h]
        up, down, far = (p + 1) % 4, (p + 3) % 4, (p + 2) % 4
        low, high = pl.ds(0, LOW), pl.ds(LOW, HIGH)
        src = part.at[m, h]
        ss, rs = s1_send.at[m, h], s1_recv.at[m, h]
        return (
            remote(src.at[far, low], lo2.at[m, h], ss.at[0], rs.at[0], dev(1)),
            remote(src.at[far, high], hi2.at[m, h], ss.at[1], rs.at[1], dev(3)),
            remote(src.at[up, high], hid.at[m, h], ss.at[2], rs.at[2], dev(1)),
            remote(src.at[down, low], lod.at[m, h], ss.at[3], rs.at[3], dev(3)),
        )

    def relay_copies(m, h):
        p, dev = firsts[h]
        ss, rs = s1_send.at[m, h], s1_recv.at[m, h]
        return (
            remote(lo2.at[m, h], los.at[m, h], ss.at[4], rs.at[4], dev(1)),
            remote(hi2.at[m, h], his.at[m, h], ss.at[5], rs.at[5], dev(3)),
        )

    def second_copies(m, h):
        p, dev = seconds[h]
        return [
            remote(
                piece.at[m, h, (p + k) % 4],
                piece_in.at[m, h, k - 1],
                s2_send.at[m, h, k - 1],
                s2_recv.at[m, h, k - 1],
                dev(k),
            )
            for k in (2, 1, 3)
        ]

    def gather1_copies(m, h, slot_of):
        p, dev = seconds[h]
        return [
            remote(
                heads.at[m, h, slot_of(p, k)],
                heads.at[m, h, slot_of(p, k)],
                g1_send.at[m, h, k - 1],
                g1_recv.at[m, h, k - 1],
                dev(k),
            )
            for k in (2, 1, 3)
        ]

    def gather2_copies(m, h, slot_of):
        p, dev = firsts[h]
        return [
            remote(
                lhs_in.at[m, h, slot_of(p, k)],
                lhs_in.at[m, h, slot_of(p, k)],
                g2_send.at[m, h, k - 1],
                g2_recv.at[m, h, k - 1],
                dev(k),
            )
            for k in (2, 1, 3)
        ]

    def sender_slot(p, k):
        return p

    def receiver_slot(p, k):
        return (p + 4 - k) % 4

    def gy_copies(m):
        return [
            remote(
                share.at[m, (gy + k) % 4],
                share_in.at[m, k - 1],
                gy_send.at[m, k - 1],
                gy_recv.at[m, k - 1],
                along_gy(k),
            )
            for k in (1, 2, 3)
        ]

    def x_copy_out(m, k):
        return remote(
            result.at[m], xs.at[m, gy], x_send.at[m, k], x_recv.at[m, k], (1, gx, (gy + k) % 4)
        )

    def x_copy_in(m, k):
        slot = xs.at[m, (gy + 4 - k) % 4]
        return remote(slot, slot, x_send.at[m, k], x_recv.at[m, k], (0, gx, gy))

    def project(m):
        @pl.when((m == 0) & (sec == 0))
        def _():
            for copy in x_copies:
                copy.wait()

        @pl.when(sec == 1)
        def _():
            for k in range(4):
                x_copy_in(m, k).wait_recv()

        for c in range(4):
            wide[c] = xs[m, c].astype(jnp.float32)
        for h in range(2):

            @pl.when(m == 0)
            def _(h=h):
                wq_copies[h].wait()
                wkv_copies[h].wait()

            if h == 1:
                for c in range(4):
                    swapped_rows(wide.at[c], turned.at[c])
            blocks = [(wide if h == 0 else turned)[c] for c in range(4)]
            scaled = jnp.concatenate(
                [(b * gain_ref[:, 128 * c : 128 * c + 128]).astype(jnp.bfloat16) for c, b in enumerate(blocks)],
                axis=1,
            )
            squares = sum(b * b for b in blocks[1:]) + blocks[0] * blocks[0]
            for c in range(4):
                part[m, h, c, 144:152, :] = squares[8 * c : 8 * c + 8, :]
            for col in range(5):
                width = 512 if col < 4 else 256
                weight = wq[h, :, 512 * col : 512 * col + 512] if col < 4 else wkv[h]
                sums = jnp.dot(scaled, weight, preferred_element_type=jnp.float32)
                for c in range(4):
                    for j in range(width // 128):
                        tile = 4 * col + j
                        part[m, h, c, 8 * tile : 8 * tile + 8, :] = sums[
                            8 * c : 8 * c + 8, 128 * j : 128 * j + 128
                        ]
            if h == 0:

                @pl.when(m == 0)
                def _():
                    pl.semaphore_wait(barrier, len(partners))

            for copy in first_copies(m, h):
                copy.start()

    def relay(m):
        for h in range(2):
            p, _ = firsts[h]
            a, b, _, _ = first_copies(m, h)
            a.wait_recv()
            lo2[m, h] = lo2[m, h] + part[m, h, (p + 1) % 4, 0:LOW, :]
            relay_copies(m, h)[0].start()
            b.wait_recv()
            hi2[m, h] = hi2[m, h] + part[m, h, (p + 3) % 4, LOW : LOW + HIGH, :]
            relay_copies(m, h)[1].start()

    def second(m):
        for h in range(2):
            p, _ = firsts[h]
            _, _, c, d = first_copies(m, h)
            e, f = relay_copies(m, h)
            c.wait_recv()
            d.wait_recv()
            e.wait_recv()
            whole[0:LOW, :] = part[m, h, p, 0:LOW, :] + lod[m, h] + los[m, h]
            f.wait_recv()
            whole[LOW : LOW + HIGH, :] = part[m, h, p, LOW : LOW + HIGH, :] + hid[m, h] + his[m, h]
            for q in range(4):
                for s in range(2):
                    piece[m, h, q, 16 * s : 16 * s + 16, :] = whole[pl.ds(2 * q + s, 16, stride=8), :]
                for i in range(3):
                    piece[m, h, q, 32 + 2 * i : 34 + 2 * i, :] = whole[
                        128 + 8 * i + 2 * q : 130 + 8 * i + 2 * q, :
                    ]
                piece[m, h, q, 38:40, :] = whole[144 + 2 * q : 146 + 2 * q, :]
            for copy in second_copies(m, h):
                copy.start()

    def attend(m):
        @pl.when(m == 0)
        def _():
            k_copy.wait()
            v_copy.wait()

        inv_scale = 1.0 / 128**0.5
        slot = lax.broadcasted_iota(jnp.int32, (16, 1024), 1)
        for h in range(2):
            p, _ = seconds[h]
            for copy in second_copies(m, h):
                copy.wait_recv()
            total[...] = piece[m, h, p] + piece_in[m, h, 0] + piece_in[m, h, 1] + piece_in[m, h, 2]
            for s in range(2):
                squares = jnp.sum(total[36 + s : 37 + s, :], axis=1, keepdims=True)
                factor = lax.rsqrt(squares / MODEL_WIDTH + NORM_EPS)
                cosine, sine = rope_ref[m, s, 0:1, :], rope_ref[m, s, 1:2, :]
                query = total[16 * s : 16 * s + 16, :] * factor
                query = (query * cosine + pltpu.roll(query, 64, 1) * sine).astype(jnp.bfloat16)
                fresh_key = total[32 + s : 33 + s, :] * factor
                fresh_key = fresh_key * cosine + pltpu.roll(fresh_key, 64, 1) * sine
                fresh_key = fresh_key.astype(jnp.bfloat16).astype(jnp.float32)
                fresh_value = (total[34 + s : 35 + s, :] * factor).astype(jnp.bfloat16).astype(jnp.float32)
                scores = (
                    lax.dot_general(
                        query,
                        keys[m, s, h],
                        (((1,), (1,)), ((), ())),
                        preferred_element_type=jnp.float32,
                    )
                    * inv_scale
                )
                own = jnp.sum(query.astype(jnp.float32) * fresh_key, axis=1, keepdims=True) * inv_scale
                scores = jnp.where(slot < len_ref[m, s], scores, -jnp.inf)
                top = jnp.maximum(jnp.max(scores, axis=1, keepdims=True), own)
                weights = jnp.exp(scores - top)
                own = jnp.exp(own - top)
                scale = 1.0 / (jnp.sum(weights, axis=1, keepdims=True) + own)
                weights = (weights * scale).astype(jnp.bfloat16)
                own = (own * scale).astype(jnp.bfloat16).astype(jnp.float32)
                mixed = jnp.dot(weights, values[m, s, h], preferred_element_type=jnp.float32)
                mixed = mixed + own * fresh_value
                heads[m, h, p, 16 * s : 16 * s + 16, :] = mixed.astype(jnp.bfloat16)
            for copy in gather1_copies(m, h, sender_slot):
                copy.start()

    def regroup(m):
        for h in range(2):
            p, _ = firsts[h]
            for copy in gather1_copies(m, h, receiver_slot):
                copy.wait_recv()
            for b in range(4):
                spread[32 * b : 32 * b + 32, :] = heads[m, h, b].astype(jnp.float32)
            for j in range(16):
                lhs_in[m, h, p, j] = spread[pl.ds(j, 8, stride=16), :].astype(jnp.bfloat16)
            for copy in gather2_copies(m, h, sender_slot):
                copy.start()

    def output(m):
        @pl.when(m == 0)
        def _():
            wo_copy.wait()

        for h in range(2):
            for copy in gather2_copies(m, h, receiver_slot):
                copy.wait_recv()
            for j in range(16):
                rows = [lhs_in[m, h, b, j].astype(jnp.float32) for b in range(4)]
                lhs[:, 128 * j : 128 * j + 128] = jnp.concatenate(rows, axis=0).astype(jnp.bfloat16)
            sums = jnp.dot(
                lhs[...], wo[2048 * h : 2048 * h + 2048, :], preferred_element_type=jnp.float32
            )
            if h == 0:
                branch0[...] = sums
            else:
                branch1[...] = sums
        swapped_rows(branch1, branch2)
        for c in range(4):
            cols = slice(128 * c, 128 * c + 128)
            share[m, c] = branch0[:, cols] + branch2[:, cols]
        for copy in gy_copies(m):
            copy.start()

    def finish(m):
        for copy in gy_copies(m):
            copy.wait_recv()
        branch = share[m, gy] + share_in[m, 0] + share_in[m, 1] + share_in[m, 2]
        state = (xs[m, gy].astype(jnp.float32) + branch).astype(jnp.bfloat16)
        out_ref[m] = state

        @pl.when(sec == 0)
        def _():
            result[m] = state
            for k in range(4):
                x_copy_out(m, k).start()

    def moment(t, carry):
        for n, stage in enumerate((project, relay, second, attend, regroup, output, finish)):
            m = t - n

            @pl.when((m >= 0) & (m < MICRO))
            def _(stage=stage, m=m):
                stage(m)

        return carry

    lax.fori_loop(0, MICRO + STAGES - 1, moment, 0)

    def settle(m, carry):
        for h in range(2):
            for copy in (
                *first_copies(m, h),
                *relay_copies(m, h),
                *second_copies(m, h),
                *gather1_copies(m, h, sender_slot),
                *gather2_copies(m, h, sender_slot),
            ):
                copy.wait_send()
        for copy in gy_copies(m):
            copy.wait_send()

        @pl.when(sec == 0)
        def _():
            for k in range(4):
                x_copy_out(m, k).wait_send()

        return carry

    lax.fori_loop(0, MICRO, settle, 0)


def body(inputs, gains, query_weight, key_value_weight, output_weight, key_cache, value_cache, lengths):
    half = 64
    frequency = ROPE_THETA ** (-2.0 * jnp.arange(half, dtype=jnp.float32) / 128)
    angles = lengths.astype(jnp.float32)[:, :, None] * frequency
    cosine, sine = jnp.cos(angles), jnp.sin(angles)
    rope = jnp.stack(
        [jnp.concatenate([cosine, cosine], axis=-1), jnp.concatenate([-sine, sine], axis=-1)], axis=2
    )
    f32, bf16 = jnp.float32, jnp.bfloat16
    vmem, anywhere = pl.BlockSpec(memory_space=pltpu.VMEM), pl.BlockSpec(memory_space=pl.ANY)
    dma = pltpu.SemaphoreType.DMA
    low, high = pltpu.VMEM((4, 2, LOW, 128), f32), pltpu.VMEM((4, 2, HIGH, 128), f32)
    states = pl.pallas_call(
        kernel,
        out_shape=jax.ShapeDtypeStruct((MICRO, ROWS, 128), bf16),
        in_specs=[anywhere, vmem, vmem, pl.BlockSpec(memory_space=pltpu.SMEM)] + [anywhere] * 5,
        out_specs=vmem,
        scratch_shapes=[
            pltpu.VMEM((4, 4, ROWS, 128), bf16),
            pltpu.VMEM((2, 512, 2048), bf16),
            pltpu.VMEM((2, 512, 256), bf16),
            pltpu.VMEM((4096, 512), bf16),
            pltpu.VMEM((4, 2, 2, 1024, 128), bf16),
            pltpu.VMEM((4, 2, 2, 1024, 128), bf16),
            pltpu.VMEM((4, ROWS, 128), f32),
            pltpu.VMEM((4, ROWS, 128), f32),
            pltpu.VMEM((4, 2, 4, 8 * TILES, 128), f32),
            low,
            low,
            low,
            high,
            high,
            high,
            pltpu.VMEM((8 * TILES, 128), f32),
            pltpu.VMEM((4, 2, 4, 40, 128), f32),
            pltpu.VMEM((4, 2, 3, 40, 128), f32),
            pltpu.VMEM((40, 128), f32),
            pltpu.VMEM((4, 2, 4, 32, 128), bf16),
            pltpu.VMEM((128, 128), f32),
            pltpu.VMEM((4, 2, 4, 16, 8, 128), bf16),
            pltpu.VMEM((ROWS, 2048), bf16),
            pltpu.VMEM((ROWS, 512), f32),
            pltpu.VMEM((ROWS, 512), f32),
            pltpu.VMEM((ROWS, 512), f32),
            pltpu.VMEM((4, 4, ROWS, 128), f32),
            pltpu.VMEM((4, 3, ROWS, 128), f32),
            pltpu.VMEM((4, ROWS, 128), bf16),
            dma((11,)),
            dma((4, 2, 6)),
            dma((4, 2, 6)),
            dma((4, 2, 3)),
            dma((4, 2, 3)),
            dma((4, 2, 3)),
            dma((4, 2, 3)),
            dma((4, 2, 3)),
            dma((4, 2, 3)),
            dma((4, 3)),
            dma((4, 3)),
            dma((4, 4)),
            dma((4, 4)),
        ],
        compiler_params=pltpu.CompilerParams(
            collective_id=0, has_side_effects=True, vmem_limit_bytes=56 * 1024 * 1024
        ),
        name="relay_layers",
    )(
        inputs,
        gains.astype(f32),
        rope,
        lengths,
        query_weight,
        key_value_weight,
        output_weight,
        key_cache,
        value_cache,
    )
    return states[None]


def solution(mesh):
    in_specs = (
        P(None, None, "gx"),
        P("section", "gx"),
        P("section", "gx", "gy"),
        P("section", "gx", "gy"),
        P("section", "gy", "gx"),
        P("section", None, "gx", "gy", None, None),
        P("section", None, "gx", "gy", None, None),
        P(None, "gx"),
    )
    out_specs = P("section", None, None, ("gx", "gy"))
    return jax.shard_map(body, mesh=mesh, in_specs=in_specs, out_specs=out_specs, check_vma=False)
```

```python
import jax
import jax.numpy as jnp
import numpy as np
from jax import lax
from jax.experimental import pallas as pl
from jax.experimental.pallas import tpu as pltpu
from jax.sharding import PartitionSpec as P

MODEL_WIDTH = 8192
ROPE_THETA = 500000.0
NORM_EPS = 1e-05

MESH = pl.DeviceIdType.MESH
MICRO = 4
ROWS = 32
TILES = 19
LOW = 80
HIGH = 72
STAGES = 7
SENT_ROWS = 1728


def swapped_rows(src, dst):
    for a in range(4):
        for b in range(4):
            dst[8 * b + 2 * a : 8 * b + 2 * a + 2, :] = src[8 * a + 2 * b : 8 * a + 2 * b + 2, :]


def kernel(
    x_hbm,
    gain_hbm,
    freq_hbm,
    len_hbm,
    wq_hbm,
    wkv_hbm,
    wo_hbm,
    k_hbm,
    v_hbm,
    out_hbm,
    gain_in,
    freq_in,
    len_ref,
    gain_ref,
    rope_ref,
    sent,
    xs,
    wq,
    wkv,
    wo,
    keys,
    values,
    wide,
    turned,
    part,
    lo2,
    lod,
    los,
    hi2,
    hid,
    his,
    whole,
    piece,
    piece_in,
    total,
    heads,
    spread,
    lhs_in,
    lhs,
    branch0,
    branch1,
    branch2,
    share,
    share_in,
    result,
    local_sem,
    send_sem,
    out_sem,
    s1_recv,
    s2_recv,
    g1_recv,
    g2_recv,
    gy_recv,
    x_send,
    x_recv,
):
    sec = lax.axis_index("section")
    gx = lax.axis_index("gx")
    gy = lax.axis_index("gy")
    z = gx // 4
    y = gx % 4

    def along_z(k):
        return (sec, ((z + k) % 4) * 4 + y, gy)

    def along_y(k):
        return (sec, z * 4 + (y + k) % 4, gy)

    def along_gy(k):
        return (sec, gx, (gy + k) % 4)

    firsts = ((z, along_z), (y, along_y))
    seconds = ((y, along_y), (z, along_z))

    def remote(src, dst, send, recv, dev):
        return pltpu.make_async_remote_copy(
            src_ref=src, dst_ref=dst, send_sem=send, recv_sem=recv, device_id=dev, device_id_type=MESH
        )

    local = []

    def stage_in(src, dst):
        copy = pltpu.make_async_copy(src, dst, local_sem.at[len(local)])
        local.append(copy)
        return copy

    small = [stage_in(gain_hbm, gain_in), stage_in(freq_hbm, freq_in), stage_in(len_hbm, len_ref)]
    x_copies = [stage_in(x_hbm.at[:, :, pl.ds(128 * c, 128)], xs.at[:, c]) for c in range(4)]
    wq_copies = []
    wkv_copies = []
    for h in range(2):
        wq_copies.append(stage_in(wq_hbm.at[0, :, pl.ds(2048 * h, 2048)], wq.at[h]))
        wkv_copies.append(stage_in(wkv_hbm.at[0, :, pl.ds(256 * h, 256)], wkv.at[h]))
    k_copy = stage_in(k_hbm.at[0], keys)
    v_copy = stage_in(v_hbm.at[0], values)
    wo_copy = stage_in(wo_hbm.at[0], wo)

    for copy in small:
        copy.start()

    @pl.when(sec == 0)
    def _():
        for copy in x_copies:
            copy.start()

    for h in range(2):
        wq_copies[h].start()
        wkv_copies[h].start()
    k_copy.start()
    v_copy.start()
    wo_copy.start()

    barrier = pltpu.get_barrier_semaphore()
    partners = [along_z(k) for k in (1, 2, 3)] + [along_y(k) for k in (1, 2, 3)]
    partners += [along_gy(k) for k in (1, 2, 3)]
    partners += [(1 - sec, gx, (gy + k) % 4) for k in range(4)]
    for dev in partners:
        pl.semaphore_signal(barrier, inc=1, device_id=dev, device_id_type=MESH)

    for copy in small:
        copy.wait()
    gain_ref[...] = gain_in[...].astype(jnp.float32)
    row = lax.broadcasted_iota(jnp.int32, (8, 128), 0)
    lane = lax.broadcasted_iota(jnp.int32, (8, 128), 1)
    spots = jnp.zeros((8, 128), jnp.int32)
    for m in range(MICRO):
        for i in range(2):
            spots = jnp.where(row == 2 * m + i, len_ref[i, m], spots)
    angles = spots.astype(jnp.float32) * freq_in[...]
    sine = jnp.sin(angles)
    rope_ref[0] = jnp.cos(angles)
    rope_ref[1] = jnp.where(lane < 64, -sine, sine)

    def first_copies(m, h):
        p, dev = firsts[h]
        up, down, far = (p + 1) % 4, (p + 3) % 4, (p + 2) % 4
        low, high = pl.ds(0, LOW), pl.ds(LOW, HIGH)
        src = part.at[m, h]
        ss, rs = send_sem.at[m], s1_recv.at[m, h]
        return (
            remote(src.at[far, low], lo2.at[m, h], ss, rs.at[0], dev(1)),
            remote(src.at[far, high], hi2.at[m, h], ss, rs.at[1], dev(3)),
            remote(src.at[up, high], hid.at[m, h], ss, rs.at[2], dev(1)),
            remote(src.at[down, low], lod.at[m, h], ss, rs.at[3], dev(3)),
        )

    def relay_copies(m, h):
        p, dev = firsts[h]
        ss, rs = send_sem.at[m], s1_recv.at[m, h]
        return (
            remote(lo2.at[m, h], los.at[m, h], ss, rs.at[4], dev(1)),
            remote(hi2.at[m, h], his.at[m, h], ss, rs.at[5], dev(3)),
        )

    def second_copies(m, h):
        p, dev = seconds[h]
        return [
            remote(
                piece.at[m, h, (p + k) % 4],
                piece_in.at[m, h, k - 1],
                send_sem.at[m],
                s2_recv.at[m, h, k - 1],
                dev(k),
            )
            for k in (2, 1, 3)
        ]

    def gather1_copies(m, h, slot_of):
        p, dev = seconds[h]
        return [
            remote(
                heads.at[m, h, slot_of(p, k)],
                heads.at[m, h, slot_of(p, k)],
                send_sem.at[m],
                g1_recv.at[m, h, k - 1],
                dev(k),
            )
            for k in (2, 1, 3)
        ]

    def gather2_copies(m, h, slot_of):
        p, dev = firsts[h]
        return [
            remote(
                lhs_in.at[m, h, slot_of(p, k)],
                lhs_in.at[m, h, slot_of(p, k)],
                send_sem.at[m],
                g2_recv.at[m, h, k - 1],
                dev(k),
            )
            for k in (2, 1, 3)
        ]

    def sender_slot(p, k):
        return p

    def receiver_slot(p, k):
        return (p + 4 - k) % 4

    def gy_copies(m):
        return [
            remote(
                share.at[m, (gy + k) % 4],
                share_in.at[m, k - 1],
                send_sem.at[m],
                gy_recv.at[m, k - 1],
                along_gy(k),
            )
            for k in (1, 2, 3)
        ]

    def x_copy_out(m, k):
        return remote(
            result.at[m], xs.at[m, gy], x_send.at[m], x_recv.at[m, k], (1, gx, (gy + k) % 4)
        )

    def x_copy_in(m, k):
        slot = xs.at[m, (gy + 4 - k) % 4]
        return remote(slot, slot, x_send.at[m], x_recv.at[m, k], (0, gx, gy))

    def project(m):
        @pl.when((m == 0) & (sec == 0))
        def _():
            for copy in x_copies:
                copy.wait()

        @pl.when(sec == 1)
        def _():
            for k in range(4):
                x_copy_in(m, k).wait_recv()

        for c in range(4):
            wide[c] = xs[m, c].astype(jnp.float32)
        for h in range(2):

            @pl.when(m == 0)
            def _(h=h):
                wq_copies[h].wait()
                wkv_copies[h].wait()

            if h == 1:
                for c in range(4):
                    swapped_rows(wide.at[c], turned.at[c])
            blocks = [(wide if h == 0 else turned)[c] for c in range(4)]
            scaled = jnp.concatenate(
                [(b * gain_ref[:, 128 * c : 128 * c + 128]).astype(jnp.bfloat16) for c, b in enumerate(blocks)],
                axis=1,
            )
            squares = sum(b * b for b in blocks[1:]) + blocks[0] * blocks[0]
            for c in range(4):
                part[m, h, c, 144:152, :] = squares[8 * c : 8 * c + 8, :]
            for col in range(5):
                width = 512 if col < 4 else 256
                weight = wq[h, :, 512 * col : 512 * col + 512] if col < 4 else wkv[h]
                sums = jnp.dot(scaled, weight, preferred_element_type=jnp.float32)
                for c in range(4):
                    for j in range(width // 128):
                        tile = 4 * col + j
                        part[m, h, c, 8 * tile : 8 * tile + 8, :] = sums[
                            8 * c : 8 * c + 8, 128 * j : 128 * j + 128
                        ]
            if h == 0:

                @pl.when(m == 0)
                def _():
                    pl.semaphore_wait(barrier, len(partners))

            for copy in first_copies(m, h):
                copy.start()

    def relay(m):
        for h in range(2):
            p, _ = firsts[h]
            a, b, _, _ = first_copies(m, h)
            a.wait_recv()
            lo2[m, h] = lo2[m, h] + part[m, h, (p + 1) % 4, 0:LOW, :]
            relay_copies(m, h)[0].start()
            b.wait_recv()
            hi2[m, h] = hi2[m, h] + part[m, h, (p + 3) % 4, LOW : LOW + HIGH, :]
            relay_copies(m, h)[1].start()

    def second(m):
        for h in range(2):
            p, _ = firsts[h]
            _, _, c, d = first_copies(m, h)
            e, f = relay_copies(m, h)
            c.wait_recv()
            d.wait_recv()
            e.wait_recv()
            whole[0:LOW, :] = part[m, h, p, 0:LOW, :] + lod[m, h] + los[m, h]
            f.wait_recv()
            whole[LOW : LOW + HIGH, :] = part[m, h, p, LOW : LOW + HIGH, :] + hid[m, h] + his[m, h]
            for q in range(4):
                for s in range(2):
                    piece[m, h, q, 16 * s : 16 * s + 16, :] = whole[pl.ds(2 * q + s, 16, stride=8), :]
                for i in range(3):
                    piece[m, h, q, 32 + 2 * i : 34 + 2 * i, :] = whole[
                        128 + 8 * i + 2 * q : 130 + 8 * i + 2 * q, :
                    ]
                piece[m, h, q, 38:40, :] = whole[144 + 2 * q : 146 + 2 * q, :]
            for copy in second_copies(m, h):
                copy.start()

    def attend(m):
        @pl.when(m == 0)
        def _():
            k_copy.wait()
            v_copy.wait()

        for h in range(2):
            for copy in second_copies(m, h):
                copy.wait_recv()
        inv_scale = 1.0 / 128**0.5
        slot = lax.broadcasted_iota(jnp.int32, (16, 1024), 1)
        pairs = [(h, i) for h in range(2) for i in range(2)]
        for h in range(2):
            p, _ = seconds[h]
            total[h] = piece[m, h, p] + piece_in[m, h, 0] + piece_in[m, h, 1] + piece_in[m, h, 2]
        queries, fresh_values, selves, scores = [], [], [], []
        for h, i in pairs:
            squares = jnp.sum(total[h, 36 + i : 37 + i, :], axis=1, keepdims=True)
            factor = lax.rsqrt(squares / MODEL_WIDTH + NORM_EPS)
            cosine, sine = rope_ref[0, pl.ds(2 * m + i, 1), :], rope_ref[1, pl.ds(2 * m + i, 1), :]
            query = total[h, 16 * i : 16 * i + 16, :] * factor
            query = (query * cosine + pltpu.roll(query, 64, 1) * sine).astype(jnp.bfloat16)
            fresh_key = total[h, 32 + i : 33 + i, :] * factor
            fresh_key = fresh_key * cosine + pltpu.roll(fresh_key, 64, 1) * sine
            fresh_key = fresh_key.astype(jnp.bfloat16).astype(jnp.float32)
            fresh_value = total[h, 34 + i : 35 + i, :] * factor
            fresh_values.append(fresh_value.astype(jnp.bfloat16).astype(jnp.float32))
            selves.append(jnp.sum(query.astype(jnp.float32) * fresh_key, axis=1, keepdims=True) * inv_scale)
            queries.append(query)
        for (h, i), query in zip(pairs, queries):
            scores.append(
                lax.dot_general(
                    query, keys[m, i, h], (((1,), (1,)), ((), ())), preferred_element_type=jnp.float32
                )
            )
        weights, owns = [], []
        for (h, i), score, own in zip(pairs, scores, selves):
            score = jnp.where(slot < len_ref[i, m], score * inv_scale, -jnp.inf)
            top = jnp.maximum(jnp.max(score, axis=1, keepdims=True), own)
            weight = jnp.exp(score - top)
            own = jnp.exp(own - top)
            scale = 1.0 / (jnp.sum(weight, axis=1, keepdims=True) + own)
            weights.append((weight * scale).astype(jnp.bfloat16))
            owns.append((own * scale).astype(jnp.bfloat16).astype(jnp.float32))
        mixes = [
            jnp.dot(weight, values[m, i, h], preferred_element_type=jnp.float32)
            for (h, i), weight in zip(pairs, weights)
        ]
        for (h, i), mixed, own, fresh_value in zip(pairs, mixes, owns, fresh_values):
            p, _ = seconds[h]
            heads[m, h, p, 16 * i : 16 * i + 16, :] = (mixed + own * fresh_value).astype(jnp.bfloat16)
        for h in range(2):
            for copy in gather1_copies(m, h, sender_slot):
                copy.start()

    def regroup(m):
        for h in range(2):
            p, _ = firsts[h]
            for copy in gather1_copies(m, h, receiver_slot):
                copy.wait_recv()
            for b in range(4):
                spread[32 * b : 32 * b + 32, :] = heads[m, h, b].astype(jnp.float32)
            for j in range(16):
                lhs_in[m, h, p, j] = spread[pl.ds(j, 8, stride=16), :].astype(jnp.bfloat16)
            for copy in gather2_copies(m, h, sender_slot):
                copy.start()

    def output(m):
        @pl.when(m == 0)
        def _():
            wo_copy.wait()

        for h in range(2):
            for copy in gather2_copies(m, h, receiver_slot):
                copy.wait_recv()
            for j in range(16):
                rows = [lhs_in[m, h, b, j].astype(jnp.float32) for b in range(4)]
                lhs[:, 128 * j : 128 * j + 128] = jnp.concatenate(rows, axis=0).astype(jnp.bfloat16)
            sums = jnp.dot(
                lhs[...], wo[2048 * h : 2048 * h + 2048, :], preferred_element_type=jnp.float32
            )
            if h == 0:
                branch0[...] = sums
            else:
                branch1[...] = sums
        swapped_rows(branch1, branch2)
        for c in range(4):
            cols = slice(128 * c, 128 * c + 128)
            share[m, c] = branch0[:, cols] + branch2[:, cols]
        for copy in gy_copies(m):
            copy.start()

    def finish(m):
        for copy in gy_copies(m):
            copy.wait_recv()
        branch = share[m, gy] + share_in[m, 0] + share_in[m, 1] + share_in[m, 2]
        state = (xs[m, gy].astype(jnp.float32) + branch).astype(jnp.bfloat16)
        result[m] = state
        pltpu.make_async_copy(result.at[m], out_hbm.at[m], out_sem.at[m]).start()

        @pl.when(sec == 0)
        def _():
            for k in range(4):
                x_copy_out(m, k).start()

    def moment(t, carry):
        for n, stage in enumerate((project, relay, second, attend, regroup, output, finish)):
            m = t - n

            @pl.when((m >= 0) & (m < MICRO))
            def _(stage=stage, m=m):
                stage(m)

        return carry

    lax.fori_loop(0, MICRO + STAGES - 1, moment, 0)

    def settle(m, carry):
        remote(sent, sent, send_sem.at[m], out_sem.at[m], along_gy(1)).wait_send()

        @pl.when(sec == 0)
        def _():
            remote(xs.at[m], xs.at[m], x_send.at[m], out_sem.at[m], along_gy(1)).wait_send()

        pltpu.make_async_copy(result.at[m], out_hbm.at[m], out_sem.at[m]).wait()
        return carry

    lax.fori_loop(0, MICRO, settle, 0)


def body(inputs, gains, query_weight, key_value_weight, output_weight, key_cache, value_cache, lengths):
    frequency = (ROPE_THETA ** (-2.0 * (np.arange(128) % 64) / 128)).astype(np.float32)[None]
    f32, bf16 = jnp.float32, jnp.bfloat16
    anywhere = pl.BlockSpec(memory_space=pl.ANY)
    dma = pltpu.SemaphoreType.DMA
    low, high = pltpu.VMEM((4, 2, LOW, 128), f32), pltpu.VMEM((4, 2, HIGH, 128), f32)
    states = pl.pallas_call(
        kernel,
        out_shape=jax.ShapeDtypeStruct((MICRO, ROWS, 128), bf16),
        in_specs=[anywhere] * 9,
        out_specs=anywhere,
        scratch_shapes=[
            pltpu.VMEM((1, 512), bf16),
            pltpu.VMEM((1, 128), f32),
            pltpu.SMEM((2, MICRO), jnp.int32),
            pltpu.VMEM((1, 512), f32),
            pltpu.VMEM((2, 8, 128), f32),
            pltpu.VMEM((SENT_ROWS, 128), f32),
            pltpu.VMEM((4, 4, ROWS, 128), bf16),
            pltpu.VMEM((2, 512, 2048), bf16),
            pltpu.VMEM((2, 512, 256), bf16),
            pltpu.VMEM((4096, 512), bf16),
            pltpu.VMEM((4, 2, 2, 1024, 128), bf16),
            pltpu.VMEM((4, 2, 2, 1024, 128), bf16),
            pltpu.VMEM((4, ROWS, 128), f32),
            pltpu.VMEM((4, ROWS, 128), f32),
            pltpu.VMEM((4, 2, 4, 8 * TILES, 128), f32),
            low,
            low,
            low,
            high,
            high,
            high,
            pltpu.VMEM((8 * TILES, 128), f32),
            pltpu.VMEM((4, 2, 4, 40, 128), f32),
            pltpu.VMEM((4, 2, 3, 40, 128), f32),
            pltpu.VMEM((2, 40, 128), f32),
            pltpu.VMEM((4, 2, 4, 32, 128), bf16),
            pltpu.VMEM((128, 128), f32),
            pltpu.VMEM((4, 2, 4, 16, 8, 128), bf16),
            pltpu.VMEM((ROWS, 2048), bf16),
            pltpu.VMEM((ROWS, 512), f32),
            pltpu.VMEM((ROWS, 512), f32),
            pltpu.VMEM((ROWS, 512), f32),
            pltpu.VMEM((4, 4, ROWS, 128), f32),
            pltpu.VMEM((4, 3, ROWS, 128), f32),
            pltpu.VMEM((4, ROWS, 128), bf16),
            dma((14,)),
            dma((4,)),
            dma((4,)),
            dma((4, 2, 6)),
            dma((4, 2, 3)),
            dma((4, 2, 3)),
            dma((4, 2, 3)),
            dma((4, 3)),
            dma((4,)),
            dma((4, 4)),
        ],
        compiler_params=pltpu.CompilerParams(
            collective_id=0, has_side_effects=True, vmem_limit_bytes=56 * 1024 * 1024
        ),
        name="relay_layers",
    )(
        inputs,
        gains,
        jnp.asarray(frequency),
        lengths.T,
        query_weight,
        key_value_weight,
        output_weight,
        key_cache,
        value_cache,
    )
    return states[None]


def solution(mesh):
    in_specs = (
        P(None, None, "gx"),
        P("section", "gx"),
        P("section", "gx", "gy"),
        P("section", "gx", "gy"),
        P("section", "gy", "gx"),
        P("section", None, "gx", "gy", None, None),
        P("section", None, "gx", "gy", None, None),
        P(None, "gx"),
    )
    out_specs = P("section", None, None, ("gx", "gy"))
    return jax.shard_map(body, mesh=mesh, in_specs=in_specs, out_specs=out_specs, check_vma=False)
```

```python
import jax
import jax.numpy as jnp
import numpy as np
from jax import lax
from jax.experimental import pallas as pl
from jax.experimental.pallas import tpu as pltpu
from jax.sharding import PartitionSpec as P

MODEL_WIDTH = 8192
ROPE_THETA = 500000.0
NORM_EPS = 1e-05

MESH = pl.DeviceIdType.MESH
MICRO = 4
ROWS = 32
TILES = 19
LOW_TILES = 10
LOW = 8 * LOW_TILES
HIGH = 8 * (TILES - LOW_TILES)
STAGES = 7
SENT_ROWS = 1728


def swapped_rows(src, dst):
    for a in range(4):
        for b in range(4):
            dst[8 * b + 2 * a : 8 * b + 2 * a + 2, :] = src[8 * a + 2 * b : 8 * a + 2 * b + 2, :]


def kernel(
    x_hbm,
    gain_hbm,
    freq_hbm,
    len_hbm,
    wq_hbm,
    wkv_hbm,
    wo_hbm,
    k_hbm,
    v_hbm,
    out_hbm,
    gain_in,
    freq_in,
    len_ref,
    gain_ref,
    rope_ref,
    sent,
    xs,
    wq,
    wkv,
    wo,
    keys,
    values,
    wide,
    turned,
    part,
    lo2,
    lod,
    los,
    hi2,
    hid,
    his,
    whole,
    piece,
    piece_in,
    total,
    heads,
    spread,
    lhs_in,
    lhs,
    branch0,
    branch1,
    branch2,
    share,
    share_in,
    result,
    local_sem,
    send_sem,
    out_sem,
    ready_sem,
    s1_recv,
    s2_recv,
    g1_recv,
    g2_recv,
    gy_recv,
    x_send,
    x_recv,
):
    sec = lax.axis_index("section")
    gx = lax.axis_index("gx")
    gy = lax.axis_index("gy")
    z = gx // 4
    y = gx % 4

    def along_z(k):
        return (sec, ((z + k) % 4) * 4 + y, gy)

    def along_y(k):
        return (sec, z * 4 + (y + k) % 4, gy)

    def along_gy(k):
        return (sec, gx, (gy + k) % 4)

    firsts = ((z, along_z), (y, along_y))
    seconds = ((y, along_y), (z, along_z))

    def remote(src, dst, send, recv, dev):
        return pltpu.make_async_remote_copy(
            src_ref=src, dst_ref=dst, send_sem=send, recv_sem=recv, device_id=dev, device_id_type=MESH
        )

    barrier = pltpu.get_barrier_semaphore()
    partners = [along(k) for along in (along_z, along_y, along_gy) for k in (1, 2, 3)]
    for dev in partners:
        pl.semaphore_signal(barrier, inc=1, device_id=dev, device_id_type=MESH)

    @pl.when(sec == 0)
    def _():
        for k in range(4):
            pl.semaphore_signal(
                barrier, inc=1, device_id=(1, gx, (gy + k) % 4), device_id_type=MESH
            )

    local = []

    def stage_in(src, dst):
        copy = pltpu.make_async_copy(src, dst, local_sem.at[len(local)])
        local.append(copy)
        return copy

    gain_copy = stage_in(gain_hbm, gain_in)
    rope_copies = [stage_in(freq_hbm, freq_in), stage_in(len_hbm, len_ref)]
    x_copies = [stage_in(x_hbm.at[:, :, pl.ds(128 * c, 128)], xs.at[:, c]) for c in range(4)]
    low_copies, high_copies = [], []
    for h in range(2):
        cut = 128 * LOW_TILES
        low_copies.append(stage_in(wq_hbm.at[0, :, pl.ds(2048 * h, cut)], wq.at[h, :, pl.ds(0, cut)]))
        high_copies.append(
            (
                stage_in(
                    wq_hbm.at[0, :, pl.ds(2048 * h + cut, 2048 - cut)], wq.at[h, :, pl.ds(cut, 2048 - cut)]
                ),
                stage_in(wkv_hbm.at[0, :, pl.ds(256 * h, 256)], wkv.at[h]),
            )
        )
    k_copy = stage_in(k_hbm.at[0], keys)
    v_copy = stage_in(v_hbm.at[0], values)
    wo_copy = stage_in(wo_hbm.at[0], wo)

    gain_copy.start()

    @pl.when(sec == 0)
    def _():
        for copy in x_copies:
            copy.start()

    for h in range(2):
        low_copies[h].start()
        for copy in high_copies[h]:
            copy.start()
    for copy in rope_copies:
        copy.start()
    k_copy.start()
    v_copy.start()
    wo_copy.start()

    @pl.when(sec == 1)
    def _():
        pl.semaphore_wait(barrier, len(partners) + 4)
        for k in range(4):
            pl.semaphore_signal(
                ready_sem, inc=1, device_id=(0, gx, (gy + k) % 4), device_id_type=MESH
            )

    gain_copy.wait()
    gain_ref[...] = gain_in[...].astype(jnp.float32)

    def make_rope():
        for copy in rope_copies:
            copy.wait()
        row = lax.broadcasted_iota(jnp.int32, (8, 128), 0)
        lane = lax.broadcasted_iota(jnp.int32, (8, 128), 1)
        spots = jnp.zeros((8, 128), jnp.int32)
        for m in range(MICRO):
            for i in range(2):
                spots = jnp.where(row == 2 * m + i, len_ref[i, m], spots)
        angles = spots.astype(jnp.float32) * freq_in[...]
        sine = jnp.sin(angles)
        rope_ref[0] = jnp.cos(angles)
        rope_ref[1] = jnp.where(lane < 64, -sine, sine)

    def first_copies(m, h):
        p, dev = firsts[h]
        up, down, far = (p + 1) % 4, (p + 3) % 4, (p + 2) % 4
        low, high = pl.ds(0, LOW), pl.ds(LOW, HIGH)
        src = part.at[m, h]
        ss, rs = send_sem.at[m], s1_recv.at[m, h]
        return (
            remote(src.at[far, low], lo2.at[m, h], ss, rs.at[0], dev(1)),
            remote(src.at[far, high], hi2.at[m, h], ss, rs.at[1], dev(3)),
            remote(src.at[up, high], hid.at[m, h], ss, rs.at[2], dev(1)),
            remote(src.at[down, low], lod.at[m, h], ss, rs.at[3], dev(3)),
        )

    def relay_copies(m, h):
        p, dev = firsts[h]
        ss, rs = send_sem.at[m], s1_recv.at[m, h]
        return (
            remote(lo2.at[m, h], los.at[m, h], ss, rs.at[4], dev(1)),
            remote(hi2.at[m, h], his.at[m, h], ss, rs.at[5], dev(3)),
        )

    def second_copies(m, h):
        p, dev = seconds[h]
        return [
            remote(
                piece.at[m, h, (p + k) % 4],
                piece_in.at[m, h, k - 1],
                send_sem.at[m],
                s2_recv.at[m, h, k - 1],
                dev(k),
            )
            for k in (2, 1, 3)
        ]

    def gather1_copies(m, h, slot_of):
        p, dev = seconds[h]
        return [
            remote(
                heads.at[m, h, slot_of(p, k)],
                heads.at[m, h, slot_of(p, k)],
                send_sem.at[m],
                g1_recv.at[m, h, k - 1],
                dev(k),
            )
            for k in (2, 1, 3)
        ]

    def gather2_copies(m, h, slot_of):
        p, dev = firsts[h]
        return [
            remote(
                lhs_in.at[m, h, slot_of(p, k)],
                lhs_in.at[m, h, slot_of(p, k)],
                send_sem.at[m],
                g2_recv.at[m, h, k - 1],
                dev(k),
            )
            for k in (2, 1, 3)
        ]

    def sender_slot(p, k):
        return p

    def receiver_slot(p, k):
        return (p + 4 - k) % 4

    def gy_copy(m, k, far):
        peer = (2 * (1 - gy // 2) + k - 2) if far else 4 * (gy // 2) + 1 - gy
        slot = (1 + gy % 2) if far else 0
        return remote(
            share.at[m, peer], share_in.at[m, slot], send_sem.at[m], gy_recv.at[m, slot], (sec, gx, peer)
        )

    def gy_arrival(m, slot):
        ref = share_in.at[m, slot]
        return remote(ref, ref, send_sem.at[m], gy_recv.at[m, slot], along_gy(1))

    def x_copy_out(m, k):
        return remote(
            result.at[m], xs.at[m, gy], x_send.at[m], x_recv.at[m, k], (1, gx, (gy + k) % 4)
        )

    def x_copy_in(m, k):
        slot = xs.at[m, (gy + 4 - k) % 4]
        return remote(slot, slot, x_send.at[m], x_recv.at[m, k], (0, gx, gy))

    def project(m, opening=False):
        if opening:

            @pl.when(sec == 0)
            def _():
                for copy in x_copies:
                    copy.wait()

        @pl.when(sec == 1)
        def _():
            for k in range(4):
                x_copy_in(m, k).wait_recv()

        for c in range(4):
            wide[c] = xs[m, c].astype(jnp.float32)
        for h in range(2):
            if h == 1:
                for c in range(4):
                    swapped_rows(wide.at[c], turned.at[c])
            blocks = [(wide if h == 0 else turned)[c] for c in range(4)]
            scaled = jnp.concatenate(
                [(b * gain_ref[:, 128 * c : 128 * c + 128]).astype(jnp.bfloat16) for c, b in enumerate(blocks)],
                axis=1,
            )

            def multiply(weight, tile, h=h, scaled=scaled):
                sums = jnp.dot(scaled, weight, preferred_element_type=jnp.float32)
                for c in range(4):
                    for j in range(weight.shape[1] // 128):
                        part[m, h, c, 8 * (tile + j) : 8 * (tile + j) + 8, :] = sums[
                            8 * c : 8 * c + 8, 128 * j : 128 * j + 128
                        ]

            squares = sum(b * b for b in blocks[1:]) + blocks[0] * blocks[0]
            for c in range(4):
                part[m, h, c, 144:152, :] = squares[8 * c : 8 * c + 8, :]
            lo_up, hi_down, hi_up, lo_down = first_copies(m, h)
            if opening:
                low_copies[h].wait()
                multiply(wq[h, :, 0:768], 0)
                multiply(wq[h, :, 768 : 128 * LOW_TILES], 6)
                if h == 0:

                    @pl.when(sec == 0)
                    def _():
                        pl.semaphore_wait(barrier, len(partners))

                lo_up.start()
                lo_down.start()
                for copy in high_copies[h]:
                    copy.wait()
                multiply(wq[h, :, 128 * LOW_TILES : 2048], LOW_TILES)
                multiply(wkv[h], 16)
            else:
                for col in range(4):
                    multiply(wq[h, :, 512 * col : 512 * col + 512], 4 * col)
                multiply(wkv[h], 16)
                lo_up.start()
                lo_down.start()
            hi_down.start()
            hi_up.start()

    def relay(m):
        for h in range(2):
            p, _ = firsts[h]
            a, b, _, _ = first_copies(m, h)
            a.wait_recv()
            lo2[m, h] = lo2[m, h] + part[m, h, (p + 1) % 4, 0:LOW, :]
            relay_copies(m, h)[0].start()
            b.wait_recv()
            hi2[m, h] = hi2[m, h] + part[m, h, (p + 3) % 4, LOW : LOW + HIGH, :]
            relay_copies(m, h)[1].start()

    def second(m):
        for h in range(2):
            p, _ = firsts[h]
            _, _, c, d = first_copies(m, h)
            e, f = relay_copies(m, h)
            c.wait_recv()
            d.wait_recv()
            e.wait_recv()
            whole[0:LOW, :] = part[m, h, p, 0:LOW, :] + lod[m, h] + los[m, h]
            f.wait_recv()
            whole[LOW : LOW + HIGH, :] = part[m, h, p, LOW : LOW + HIGH, :] + hid[m, h] + his[m, h]
            for q in range(4):
                for s in range(2):
                    piece[m, h, q, 16 * s : 16 * s + 16, :] = whole[pl.ds(2 * q + s, 16, stride=8), :]
                for i in range(3):
                    piece[m, h, q, 32 + 2 * i : 34 + 2 * i, :] = whole[
                        128 + 8 * i + 2 * q : 130 + 8 * i + 2 * q, :
                    ]
                piece[m, h, q, 38:40, :] = whole[144 + 2 * q : 146 + 2 * q, :]
            for copy in second_copies(m, h):
                copy.start()

    def attend(m):
        @pl.when(m == 0)
        def _():
            k_copy.wait()
            v_copy.wait()

        for h in range(2):
            for copy in second_copies(m, h):
                copy.wait_recv()
        inv_scale = 1.0 / 128**0.5
        slot = lax.broadcasted_iota(jnp.int32, (16, 1024), 1)
        pairs = [(h, i) for h in range(2) for i in range(2)]
        for h in range(2):
            p, _ = seconds[h]
            total[h] = piece[m, h, p] + piece_in[m, h, 0] + piece_in[m, h, 1] + piece_in[m, h, 2]
        queries, fresh_values, selves, scores = [], [], [], []
        for h, i in pairs:
            squares = jnp.sum(total[h, 36 + i : 37 + i, :], axis=1, keepdims=True)
            factor = lax.rsqrt(squares / MODEL_WIDTH + NORM_EPS)
            cosine, sine = rope_ref[0, pl.ds(2 * m + i, 1), :], rope_ref[1, pl.ds(2 * m + i, 1), :]
            query = total[h, 16 * i : 16 * i + 16, :] * factor
            query = (query * cosine + pltpu.roll(query, 64, 1) * sine).astype(jnp.bfloat16)
            fresh_key = total[h, 32 + i : 33 + i, :] * factor
            fresh_key = fresh_key * cosine + pltpu.roll(fresh_key, 64, 1) * sine
            fresh_key = fresh_key.astype(jnp.bfloat16).astype(jnp.float32)
            fresh_value = total[h, 34 + i : 35 + i, :] * factor
            fresh_values.append(fresh_value.astype(jnp.bfloat16).astype(jnp.float32))
            selves.append(jnp.sum(query.astype(jnp.float32) * fresh_key, axis=1, keepdims=True) * inv_scale)
            queries.append(query)
        for (h, i), query in zip(pairs, queries):
            scores.append(
                lax.dot_general(
                    query, keys[m, i, h], (((1,), (1,)), ((), ())), preferred_element_type=jnp.float32
                )
            )
        weights, owns = [], []
        for (h, i), score, own in zip(pairs, scores, selves):
            score = jnp.where(slot < len_ref[i, m], score * inv_scale, -jnp.inf)
            top = jnp.maximum(jnp.max(score, axis=1, keepdims=True), own)
            weight = jnp.exp(score - top)
            own = jnp.exp(own - top)
            scale = 1.0 / (jnp.sum(weight, axis=1, keepdims=True) + own)
            weights.append((weight * scale).astype(jnp.bfloat16))
            owns.append((own * scale).astype(jnp.bfloat16).astype(jnp.float32))
        mixes = [
            jnp.dot(weight, values[m, i, h], preferred_element_type=jnp.float32)
            for (h, i), weight in zip(pairs, weights)
        ]
        for (h, i), mixed, own, fresh_value in zip(pairs, mixes, owns, fresh_values):
            p, _ = seconds[h]
            heads[m, h, p, 16 * i : 16 * i + 16, :] = (mixed + own * fresh_value).astype(jnp.bfloat16)
        for h in range(2):
            for copy in gather1_copies(m, h, sender_slot):
                copy.start()

    def regroup(m):
        for h in range(2):
            p, _ = firsts[h]
            for copy in gather1_copies(m, h, receiver_slot):
                copy.wait_recv()
            for b in range(4):
                spread[32 * b : 32 * b + 32, :] = heads[m, h, b].astype(jnp.float32)
            for j in range(16):
                lhs_in[m, h, p, j] = spread[pl.ds(j, 8, stride=16), :].astype(jnp.bfloat16)
            for copy in gather2_copies(m, h, sender_slot):
                copy.start()

    def output(m):
        @pl.when(m == 0)
        def _():
            wo_copy.wait()

        for h in range(2):
            for copy in gather2_copies(m, h, receiver_slot):
                copy.wait_recv()
            for j in range(16):
                rows = [lhs_in[m, h, b, j].astype(jnp.float32) for b in range(4)]
                lhs[h, :, 128 * j : 128 * j + 128] = jnp.concatenate(rows, axis=0).astype(jnp.bfloat16)
        near = gy // 2
        for side in (1 - near, near):
            cols = pl.ds(pl.multiple_of(256 * side, 256), 256)
            branch0[...] = jnp.dot(lhs[0], wo[0:2048, cols], preferred_element_type=jnp.float32)
            branch1[...] = jnp.dot(lhs[1], wo[2048:4096, cols], preferred_element_type=jnp.float32)
            swapped_rows(branch1, branch2)
            for c in range(2):
                share[m, 2 * side + c] = (
                    branch0[:, 128 * c : 128 * c + 128] + branch2[:, 128 * c : 128 * c + 128]
                )
            if side is not near:
                for k in (2, 3):
                    gy_copy(m, k, far=True).start()
        gy_copy(m, 1, far=False).start()

    def finish(m):
        for slot in range(3):
            gy_arrival(m, slot).wait_recv()
        branch = share[m, gy] + share_in[m, 0] + share_in[m, 1] + share_in[m, 2]
        state = (xs[m, gy].astype(jnp.float32) + branch).astype(jnp.bfloat16)
        result[m] = state
        pltpu.make_async_copy(result.at[m], out_hbm.at[m], out_sem.at[m]).start()

        @pl.when((sec == 0) & (m == 0))
        def _():
            pl.semaphore_wait(ready_sem, 4)

        @pl.when(sec == 0)
        def _():
            for k in range(4):
                x_copy_out(m, k).start()

    def moment(t, carry):
        for n, stage in ((0, project), (2, relay), (4, second), (6, attend), (8, regroup), (10, output), (12, finish)):
            m = t - n

            @pl.when((m >= (1 if n == 0 else 0)) & (m < MICRO))
            def _(stage=stage, m=m):
                stage(m)

        return carry

    project(0, opening=True)
    make_rope()
    lax.fori_loop(1, MICRO + 12, moment, 0)

    def settle(m, carry):
        remote(sent, sent, send_sem.at[m], out_sem.at[m], along_gy(1)).wait_send()

        @pl.when(sec == 0)
        def _():
            remote(xs.at[m], xs.at[m], x_send.at[m], out_sem.at[m], along_gy(1)).wait_send()

        pltpu.make_async_copy(result.at[m], out_hbm.at[m], out_sem.at[m]).wait()
        return carry

    lax.fori_loop(0, MICRO, settle, 0)


def body(inputs, gains, query_weight, key_value_weight, output_weight, key_cache, value_cache, lengths):
    frequency = (ROPE_THETA ** (-2.0 * (np.arange(128) % 64) / 128)).astype(np.float32)[None]
    f32, bf16 = jnp.float32, jnp.bfloat16
    anywhere = pl.BlockSpec(memory_space=pl.ANY)
    dma = pltpu.SemaphoreType.DMA
    low, high = pltpu.VMEM((4, 2, LOW, 128), f32), pltpu.VMEM((4, 2, HIGH, 128), f32)
    states = pl.pallas_call(
        kernel,
        out_shape=jax.ShapeDtypeStruct((MICRO, ROWS, 128), bf16),
        in_specs=[anywhere] * 9,
        out_specs=anywhere,
        scratch_shapes=[
            pltpu.VMEM((1, 512), bf16),
            pltpu.VMEM((1, 128), f32),
            pltpu.SMEM((2, MICRO), jnp.int32),
            pltpu.VMEM((1, 512), f32),
            pltpu.VMEM((2, 8, 128), f32),
            pltpu.VMEM((SENT_ROWS, 128), f32),
            pltpu.VMEM((4, 4, ROWS, 128), bf16),
            pltpu.VMEM((2, 512, 2048), bf16),
            pltpu.VMEM((2, 512, 256), bf16),
            pltpu.VMEM((4096, 512), bf16),
            pltpu.VMEM((4, 2, 2, 1024, 128), bf16),
            pltpu.VMEM((4, 2, 2, 1024, 128), bf16),
            pltpu.VMEM((4, ROWS, 128), f32),
            pltpu.VMEM((4, ROWS, 128), f32),
            pltpu.VMEM((4, 2, 4, 8 * TILES, 128), f32),
            low,
            low,
            low,
            high,
            high,
            high,
            pltpu.VMEM((8 * TILES, 128), f32),
            pltpu.VMEM((4, 2, 4, 40, 128), f32),
            pltpu.VMEM((4, 2, 3, 40, 128), f32),
            pltpu.VMEM((2, 40, 128), f32),
            pltpu.VMEM((4, 2, 4, 32, 128), bf16),
            pltpu.VMEM((128, 128), f32),
            pltpu.VMEM((4, 2, 4, 16, 8, 128), bf16),
            pltpu.VMEM((2, ROWS, 2048), bf16),
            pltpu.VMEM((ROWS, 256), f32),
            pltpu.VMEM((ROWS, 256), f32),
            pltpu.VMEM((ROWS, 256), f32),
            pltpu.VMEM((4, 4, ROWS, 128), f32),
            pltpu.VMEM((4, 3, ROWS, 128), f32),
            pltpu.VMEM((4, ROWS, 128), bf16),
            dma((16,)),
            dma((4,)),
            dma((4,)),
            pltpu.SemaphoreType.REGULAR,
            dma((4, 2, 6)),
            dma((4, 2, 3)),
            dma((4, 2, 3)),
            dma((4, 2, 3)),
            dma((4, 3)),
            dma((4,)),
            dma((4, 4)),
        ],
        compiler_params=pltpu.CompilerParams(
            collective_id=0, has_side_effects=True, vmem_limit_bytes=56 * 1024 * 1024
        ),
        name="relay_layers",
    )(
        inputs,
        gains,
        jnp.asarray(frequency),
        lengths.T,
        query_weight,
        key_value_weight,
        output_weight,
        key_cache,
        value_cache,
    )
    return states[None]


def solution(mesh):
    in_specs = (
        P(None, None, "gx"),
        P("section", "gx"),
        P("section", "gx", "gy"),
        P("section", "gx", "gy"),
        P("section", "gy", "gx"),
        P("section", None, "gx", "gy", None, None),
        P("section", None, "gx", "gy", None, None),
        P(None, "gx"),
    )
    out_specs = P("section", None, None, ("gx", "gy"))
    return jax.shard_map(body, mesh=mesh, in_specs=in_specs, out_specs=out_specs, check_vma=False)
```
